32 devices in a mesh: gx: 8 (over y, x, core), gy: 4 (over z).
Axes of the slice: x: 2, y: 2, z: 4, core: 2. Of those that a mesh axis runs over, the one named last changes fastest.
Arguments:
- patches: bfloat16 [256, 8192], P('gy', 'gx'), may hold values from -400 to 400, as said below
- norm_gain: bfloat16 [8192], P('gx'), may hold values from 0.099609375 to 1.8984375
- gate_weight: bfloat16 [8192, 28672], P('gx', 'gy'), may hold values from -0.0625 to 0.0625
- up_weight: bfloat16 [8192, 28672], P('gx', 'gy'), may hold values from -0.0625 to 0.0625
- down_weight: bfloat16 [28672, 8192], P('gy', 'gx'), may hold values from -0.03125 to 0.03125
Outputs:
- block_out: bfloat16 [256, 8192], P('gy', 'gx')
The draws below stay inside these ranges and needn't reach their ends.
Inputs may be any that keep to these rules, and one draw needn't show every extreme that they name: `patches`: real-valued activations of a pooled encoder.
All inputs are finite; a program needn't handle non-finite values.
Results may differ from the reference program's by a relative error of at most 0.0065.
Values may be sent and summed in bfloat16 or wider, within the bound.
No kernel may reach another device: no remote copies, remote signals or barrier semaphores. Data moves between devices by JAX's collectives and lax.ppermute only.
A program may use at most 128 MiB of HBM per device.

```python
import jax
import jax.numpy as jnp
from jax import lax

D = 8192
FF = 28672
TOK = 256


def draw_patches(key, part):
    keys = jax.random.split(jax.random.fold_in(key, 17), 3)
    offsets = jax.random.uniform(keys[1], (1, D), minval=-0.25, maxval=0.25)
    columns = 10.0 ** (0.5 * jnp.arange(D, dtype=jnp.float32)[None, :] / D + offsets)
    row_scale = 10.0 ** jax.random.uniform(keys[0], (TOK, 1))
    base = jnp.clip(jax.random.normal(keys[2], (TOK, D)), -6.0, 6.0)
    return (base * row_scale * columns).astype(jnp.bfloat16)


def block_scale(key, shape, cuts, smallest, high):
    factor_of = 1.0
    for position, shards_of in cuts:
        draws = jax.random.uniform(jax.random.fold_in(jax.random.fold_in(key, 6), position), (shards_of,), jnp.float32, smallest / len(cuts), high / len(cuts))
        factor_of = factor_of * jnp.repeat(jnp.exp(draws), shape[position] // shards_of).reshape((-1,) + (1,) * (len(shape) - 1 - position))
    return factor_of


def noise(own_key, dims, scale, most, cuts=(), kind=jnp.bfloat16):
    array = jax.random.normal(own_key, dims, jnp.float32) * scale
    if len(cuts) > 0:
        array = block_scale(own_key, dims, cuts, -0.22, 0.18) * array
    return jnp.clip(array, min=-most, max=most).astype(kind)


def setup_inputs(seed: int = 0) -> dict:
    streams_of = jax.random.split(jax.random.key(seed), 6)
    patches = draw_patches(jax.random.fold_in(streams_of[5], 71), 0)
    norm_gain = jnp.clip(1.0 + 0.18 * jax.random.normal(streams_of[1], (D,), jnp.float32), 0.099609375, 1.8984375).astype(jnp.bfloat16)
    gate_weight = noise(streams_of[2], (D, FF), D ** -0.5, 0.0625, ((0, 8), (1, 4)))
    up_weight = noise(streams_of[3], (D, FF), D ** -0.5, 0.0625, ((0, 8), (1, 4)))
    down_weight = noise(streams_of[4], (FF, D), FF ** -0.5, 0.03125, ((0, 4), (1, 8)))
    return dict(patches=patches, norm_gain=norm_gain, gate_weight=gate_weight, up_weight=up_weight, down_weight=down_weight)


EPS = 1e-05

def reference(patches, norm_gain, gate_weight, up_weight, down_weight):
    values = patches.astype(jnp.float32)
    mean_sq = lax.optimization_barrier(jnp.mean(values * values, axis=1))
    normed = (values * lax.rsqrt(mean_sq + EPS)[:, None] * norm_gain.astype(jnp.float32)[None, :]).astype(jnp.bfloat16)
    gate = jnp.dot(normed, gate_weight, preferred_element_type=jnp.float32)
    up = jnp.dot(normed, up_weight, preferred_element_type=jnp.float32)
    hidden = (jax.nn.silu(gate) * up).astype(jnp.bfloat16)
    return jnp.dot(hidden, down_weight, preferred_element_type=jnp.float32).astype(jnp.bfloat16)
```

```python
import functools

import jax
import jax.numpy as jnp
from jax import lax
from jax.experimental import pallas as pl
from jax.experimental.pallas import tpu as pltpu
from jax.sharding import PartitionSpec as P

EPS = 1e-05
TILE = 256
LANES = 128


def swiglu(sums):
    return (jax.nn.silu(sums[:, 0]) * sums[:, 1]).astype(jnp.bfloat16)


def generic(patches, norm_gain, gate_weight, up_weight, down_weight):
    values = patches.astype(jnp.float32)
    square_total = lax.psum(jnp.sum(values * values, axis=1), "gx")
    width = patches.shape[1] * lax.axis_size("gx")
    scale = lax.rsqrt(square_total / width + EPS)
    normed = (values * scale[:, None] * norm_gain.astype(jnp.float32)[None, :]).astype(jnp.bfloat16)
    whole = lax.all_gather(normed, "gy", axis=0, tiled=True)
    gate = jnp.dot(whole, gate_weight, preferred_element_type=jnp.float32)
    up = jnp.dot(whole, up_weight, preferred_element_type=jnp.float32)
    sums = lax.psum_scatter(jnp.stack([gate, up], axis=1), "gx", scatter_dimension=2, tiled=True)
    hidden = swiglu(sums)
    partial_value = jnp.dot(
        lax.all_gather(hidden, "gx", axis=1, tiled=True),
        down_weight,
        preferred_element_type=jnp.float32,
    )
    return lax.psum_scatter(partial_value, "gy", scatter_dimension=0, tiled=True).astype(
        jnp.bfloat16
    )


def first_bit(core):
    return 2 + 2 * core


def second_bit(core):
    return 4 - 2 * core


def owner(me, p):
    c, a, b = (p >> 2) & 1, (p >> 1) & 1, p & 1
    core = (me & 1) ^ c
    return me ^ c ^ (a * first_bit(core)) ^ (b * second_bit(core))


def position(me, j):
    c = (j ^ me) & 1
    core = j & 1
    diff = j ^ me ^ c
    shift_first, shift_second = 1 + core, 2 - core
    return c * 4 + ((diff >> shift_first) & 1) * 2 + ((diff >> shift_second) & 1)


def swap(a, stage, n):
    if stage == 0:
        pairs = [(i, i ^ 1) for i in range(n)]
    elif stage == 1:
        pairs = [(i, i ^ first_bit(i & 1)) for i in range(n)]
    else:
        pairs = [(i, i ^ second_bit(i & 1)) for i in range(n)]
    return lax.ppermute(a, "gx", pairs)


def up_kernel(extra, nt, *refs):
    parts, (gain, gw, uw, send, keep, lhs) = refs[:-6], refs[-6:]
    depth, rows = len(parts), parts[0].shape[0]
    half = rows // 2
    j = pl.program_id(0)

    @pl.when(j == 0)
    def _():
        for d in range(depth):
            v = parts[d][...].astype(jnp.float32)
            lhs[d * rows : (d + 1) * rows, :] = (v * gain[...].astype(jnp.float32)).astype(
                jnp.bfloat16
            )

    @pl.when(j < nt)
    def _():
        for k, w in enumerate((gw, uw)):
            out = jnp.dot(lhs[...], w[...], preferred_element_type=jnp.float32)
            for d in range(depth):
                keep[k, d] = out[d * rows : d * rows + half]
                send[k, d] = out[d * rows + half : (d + 1) * rows].astype(jnp.bfloat16)

    if extra:

        @pl.when(j == nt)
        def _():
            for d in range(depth):
                v = parts[d][...].astype(jnp.float32)
                total = jnp.sum(v * v, axis=1, keepdims=True)
                total = jnp.broadcast_to(total, (rows, TILE))
                for k in range(2):
                    keep[k, d] = total[:half]
                    send[k, d] = total[half:].astype(jnp.bfloat16)


def up_call(parts, gain, gw, uw, start, width, extra):
    rows, feat = parts[0].shape
    depth, half, nt = len(parts), rows // 2, width // TILE
    cols = width + (LANES if extra else 0)
    first = start // TILE
    weights = pl.BlockSpec((feat, TILE), lambda j: (0, first + jnp.minimum(j, nt - 1)))
    out = pl.BlockSpec((2, depth, half, TILE), lambda j: (0, 0, 0, j))
    full = lambda *shape: pl.BlockSpec(shape, lambda j: (0,) * len(shape))
    return pl.pallas_call(
        functools.partial(up_kernel, extra, nt),
        grid=(nt + (1 if extra else 0),),
        in_specs=[full(rows, feat)] * depth + [full(1, feat), weights, weights],
        out_specs=[out, out],
        out_shape=[
            jax.ShapeDtypeStruct((2, depth, half, cols), jnp.bfloat16),
            jax.ShapeDtypeStruct((2, depth, half, cols), jnp.float32),
        ],
        scratch_shapes=[pltpu.VMEM((depth * rows, feat), jnp.bfloat16)],
        compiler_params=pltpu.CompilerParams(
            dimension_semantics=("arbitrary",), vmem_limit_bytes=24 << 20
        ),
        cost_estimate=pl.CostEstimate(
            flops=4 * depth * rows * feat * width,
            bytes_accessed=4 * feat * width + 12 * depth * half * width,
            transcendentals=0,
        ),
        name="gate_up",
    )(*parts, gain, gw, uw)


def down_kernel(has_acc, last, depth, *refs):
    pieces, refs = refs[:4], refs[4:]
    if has_acc:
        acc_in, refs = refs[0], refs[1:]
    dw, refs = refs[0], refs[1:]
    outs, (acc, lhs) = refs[:-2], refs[-2:]
    k = pl.program_id(0)
    sub = pieces[0].shape[1]
    rows = 4 * sub

    @pl.when(k == 0)
    def _():
        if has_acc:
            acc[...] = acc_in[...]
        else:
            acc[...] = jnp.zeros_like(acc)

    for d in range(depth):
        for q in range(4):
            at = d * rows + q * sub
            lhs[at : at + sub, :] = pieces[q][d]
    acc[...] += jnp.dot(lhs[...], dw[...], preferred_element_type=jnp.float32)

    @pl.when(k == pl.num_programs(0) - 1)
    def _():
        if last:
            outs[0][...] = acc[:rows]
            for d in range(1, depth):
                outs[d][...] = acc[d * rows : (d + 1) * rows].astype(jnp.bfloat16)
        else:
            outs[0][...] = acc[...]


def down_call(pieces, acc, dw, start, last):
    depth, sub, width = pieces[0].shape
    feat = dw.shape[1]
    rows = 4 * sub
    tile = 2 * TILE if width % (2 * TILE) == 0 and start % (2 * TILE) == 0 else TILE
    first = start // tile
    full = lambda *shape: pl.BlockSpec(shape, lambda k: (0,) * len(shape))
    if last:
        shapes = [jax.ShapeDtypeStruct((rows, feat), jnp.float32)] + [
            jax.ShapeDtypeStruct((rows, feat), jnp.bfloat16)
        ] * (depth - 1)
    else:
        shapes = [jax.ShapeDtypeStruct((depth * rows, feat), jnp.float32)]
    return pl.pallas_call(
        functools.partial(down_kernel, acc is not None, last, depth),
        grid=(width // tile,),
        in_specs=[pl.BlockSpec((depth, sub, tile), lambda k: (0, 0, k))] * 4
        + ([full(depth * rows, feat)] if acc is not None else [])
        + [pl.BlockSpec((tile, feat), lambda k: (first + k, 0))],
        out_specs=[full(*s.shape) for s in shapes],
        out_shape=shapes,
        scratch_shapes=[
            pltpu.VMEM((depth * rows, feat), jnp.float32),
            pltpu.VMEM((depth * rows, tile), jnp.bfloat16),
        ],
        compiler_params=pltpu.CompilerParams(
            dimension_semantics=("arbitrary",), vmem_limit_bytes=24 << 20
        ),
        cost_estimate=pl.CostEstimate(
            flops=2 * depth * rows * feat * width,
            bytes_accessed=2 * feat * width + 8 * depth * rows * feat,
            transcendentals=0,
        ),
        name="down",
    )(*pieces, *([acc] if acc is not None else []), dw)


def fast(cuts, n, m, patches, norm_gain, gate_weight, up_weight, down_weight):
    me = lax.axis_index("gx")
    rows, feat = patches.shape
    sub = rows // n
    features = feat * n
    blocks = patches.reshape(n, sub, feat)
    own = jnp.concatenate(
        [lax.dynamic_slice_in_dim(blocks, owner(me, p), 1, 0) for p in range(n)], axis=0
    ).reshape(rows, feat)
    parts = [own] + [
        lax.ppermute(own, "gy", [(i, i ^ d) for i in range(m)]) for d in range(1, m)
    ]
    gain = norm_gain.reshape(1, feat)

    def received(kept, *arrived):
        total = kept
        for a in arrived:
            total = total + a.astype(jnp.float32)
        return total

    start, acc, scale = 0, None, None
    for index, width in enumerate(cuts):
        extra = index == 0
        send, keep = up_call(parts, gain, gate_weight, up_weight, start, width, extra)
        r0 = swap(send, 0, n)
        h = r0.shape[2] // 2
        s1 = received(keep[:, :, h:], r0[:, :, h:]).astype(jnp.bfloat16)
        r1 = swap(s1, 1, n)
        q = h // 2
        s2 = received(keep[:, :, q:h], r0[:, :, q:h], r1[:, :, q:]).astype(jnp.bfloat16)
        r2 = swap(s2, 2, n)
        sums = received(keep[:, :, :q], r0[:, :, :q], r1[:, :, :q], r2)
        if extra:
            scale = lax.rsqrt(sums[0, :, :, width : width + 1] / features + EPS)
            sums = sums[:, :, :, :width]
        gate, up = sums[0] * scale, sums[1] * scale
        hidden = (jax.nn.silu(gate) * up).astype(jnp.bfloat16)
        g1 = swap(hidden, 2, n)
        near = jnp.concatenate([hidden, g1], axis=1)
        far = swap(near, 1, n)
        pieces = [near, far, swap(near, 0, n), swap(far, 0, n)]
        last = index == len(cuts) - 1
        outs = down_call(pieces, acc, down_weight, start, last)
        acc = outs[0]
        start += width
    total = acc
    for d in range(1, m):
        total = total + lax.ppermute(outs[d], "gy", [(i, i ^ d) for i in range(m)]).astype(
            jnp.float32
        )
    blocks = total.reshape(n, sub, -1)
    return (
        jnp.concatenate(
            [lax.dynamic_slice_in_dim(blocks, position(me, j), 1, 0) for j in range(n)], axis=0
        )
        .reshape(rows, -1)
        .astype(jnp.bfloat16)
    )


def solution(mesh):
    n, m = mesh.shape["gx"], mesh.shape["gy"]
    placed = (P("gy", "gx"), P("gx"), P("gx", "gy"), P("gx", "gy"), P("gy", "gx"))

    def per_device(patches, norm_gain, gate_weight, up_weight, down_weight):
        rows, ff = patches.shape[0], gate_weight.shape[1]
        fits = n == 8 and m in (2, 4, 8) and rows % (8 * n) == 0 and ff % (4 * TILE) == 0
        if not fits:
            return generic(patches, norm_gain, gate_weight, up_weight, down_weight)
        cuts = [ff // 4] * 4
        return fast(cuts, n, m, patches, norm_gain, gate_weight, up_weight, down_weight)

    return jax.shard_map(
        per_device, mesh=mesh, in_specs=placed, out_specs=P("gy", "gx"), check_vma=False
    )
```

```python
import functools

import jax
import jax.numpy as jnp
from jax import lax
from jax.experimental import pallas as pl
from jax.experimental.pallas import tpu as pltpu
from jax.sharding import PartitionSpec as P


EPS = 1e-05
LANES = 128
TILE = 512
VMEM_MIB = dict(up0=50, up1=50, up2=44, down1=48, down2=48)


def swiglu(sums):
    return (jax.nn.silu(sums[:, 0]) * sums[:, 1]).astype(jnp.bfloat16)


def generic(patches, norm_gain, gate_weight, up_weight, down_weight):
    values = patches.astype(jnp.float32)
    square_total = lax.psum(jnp.sum(values * values, axis=1), "gx")
    width = patches.shape[1] * lax.axis_size("gx")
    scale = lax.rsqrt(square_total / width + EPS)
    normed = (values * scale[:, None] * norm_gain.astype(jnp.float32)[None, :]).astype(jnp.bfloat16)
    whole = lax.all_gather(normed, "gy", axis=0, tiled=True)
    gate = jnp.dot(whole, gate_weight, preferred_element_type=jnp.float32)
    up = jnp.dot(whole, up_weight, preferred_element_type=jnp.float32)
    sums = lax.psum_scatter(jnp.stack([gate, up], axis=1), "gx", scatter_dimension=2, tiled=True)
    hidden = swiglu(sums)
    partial_value = jnp.dot(
        lax.all_gather(hidden, "gx", axis=1, tiled=True),
        down_weight,
        preferred_element_type=jnp.float32,
    )
    return lax.psum_scatter(partial_value, "gy", scatter_dimension=0, tiled=True).astype(
        jnp.bfloat16
    )


def first_bit(core):
    return 2 + 2 * core


def second_bit(core):
    return 4 - 2 * core


def owner(me, p):
    c, a, b = (p >> 2) & 1, (p >> 1) & 1, p & 1
    core = (me & 1) ^ c
    return me ^ c ^ (a * first_bit(core)) ^ (b * second_bit(core))


def position(me, j):
    c = (j ^ me) & 1
    core = j & 1
    diff = j ^ me ^ c
    shift_first, shift_second = 1 + core, 2 - core
    return c * 4 + ((diff >> shift_first) & 1) * 2 + ((diff >> shift_second) & 1)


def swap(a, stage, n):
    if stage == 0:
        pairs = [(i, i ^ 1) for i in range(n)]
    elif stage == 1:
        pairs = [(i, i ^ first_bit(i & 1)) for i in range(n)]
    else:
        pairs = [(i, i ^ second_bit(i & 1)) for i in range(n)]
    return lax.ppermute(a, "gx", pairs)


def take(a, shift, m):
    return lax.ppermute(a, "gy", [((i + shift) % m, i) for i in range(m)])


def up_kernel(first, count, deep, shape, build, *refs):
    depth, rows, sub = shape
    half = rows // 2
    if build:
        (offs, gain), parts, refs = refs[:2], refs[2 : 2 + depth], refs[2 + depth :]
        gw, uw, send, keep, lhs, buf, sem, wide = refs
    else:
        gw, uw, send, keep, buf, sem, lhs = refs[-7:]
        made_before = refs[:-7]

    def copies(j):
        slot = j % deep
        cols = slice((first + j) * TILE, (first + j + 1) * TILE)
        return [
            pltpu.make_async_copy(w.at[:, cols], buf.at[slot, k], sem.at[slot, k])
            for k, w in enumerate((gw, uw))
        ]

    def prepare():
        factor = gain[...].astype(jnp.float32)
        cols = slice(count * TILE, count * TILE + LANES)
        for d in range(depth):
            wide[...] = parts[d][...].astype(jnp.float32)
            for p in range(0, rows // sub, 2):
                pair = jnp.concatenate(
                    [
                        wide[pl.ds(pl.multiple_of(offs[p + e], sub), sub), :]
                        for e in range(2)
                    ],
                    axis=0,
                )
                at = p * sub
                lhs[d * rows + at : d * rows + at + 2 * sub, :] = (pair * factor).astype(
                    jnp.bfloat16
                )
                total = jnp.sum(pair * pair, axis=1, keepdims=True)
                total = jnp.broadcast_to(total, (2 * sub, LANES))
                for k in range(2):
                    if at < half:
                        keep[k, d, at : at + 2 * sub, cols] = total
                    else:
                        send[k, d, at - half : at - half + 2 * sub, cols] = total.astype(
                            send.dtype
                        )

    for j in range(min(deep, count)):
        for c in copies(j):
            c.start()
    if build:
        prepare()
    else:
        at = 0
        for ref in made_before:
            lhs[at : at + ref.shape[0], :] = ref[...]
            at += ref.shape[0]
    for j in range(count):
        for c in copies(j):
            c.wait()
        cols = slice(j * TILE, (j + 1) * TILE)
        for k in range(2):
            out = jnp.dot(lhs[...], buf[j % deep, k], preferred_element_type=jnp.float32)
            for d in range(depth):
                keep[k, d, :, cols] = out[d * rows : d * rows + half]
                send[k, d, :, cols] = out[d * rows + half : (d + 1) * rows].astype(send.dtype)
        if j + deep < count:
            for c in copies(j + deep):
                c.start()


VM = pl.BlockSpec(memory_space=pltpu.VMEM)
HBM = pl.BlockSpec(memory_space=pltpu.HBM)
SM = pl.BlockSpec(memory_space=pltpu.SMEM)


def params(name):
    return pltpu.CompilerParams(vmem_limit_bytes=VMEM_MIB.get(name, 16) << 20)


def up_call(name, inputs, gw, uw, start, width, shape, build, kind):
    depth, rows, _ = shape
    feat = gw.shape[0]
    count, half = width // TILE, rows // 2
    deep = min(count, 4)
    cols = width + (LANES if build else 0)
    outs = [
        jax.ShapeDtypeStruct((2, depth, half, cols), kind),
        jax.ShapeDtypeStruct((2, depth, half, cols), jnp.float32),
    ]
    scratch = [
        pltpu.VMEM((deep, 2, feat, TILE), jnp.bfloat16),
        pltpu.SemaphoreType.DMA((deep, 2)),
    ]
    whole = (depth * rows, feat)
    if build:
        outs.append(jax.ShapeDtypeStruct(whole, jnp.bfloat16))
        scratch.append(pltpu.VMEM((rows, feat), jnp.float32))
    else:
        scratch.append(pltpu.VMEM(whole, jnp.bfloat16))
    return pl.pallas_call(
        functools.partial(up_kernel, start // TILE, count, deep, shape, build),
        in_specs=[SM if build and k == 0 else VM for k in range(len(inputs))] + [HBM, HBM],
        out_specs=[VM] * len(outs),
        out_shape=outs,
        scratch_shapes=scratch,
        compiler_params=params(name),
        cost_estimate=pl.CostEstimate(
            flops=4 * depth * rows * feat * width,
            bytes_accessed=4 * feat * width,
            transcendentals=0,
        ),
        name="gate_up",
    )(*inputs, gw, uw)


def hidden_kernel(features, width, step, build, depth, *refs):
    keep, r0, r1, r2 = refs[:4]
    out = refs[-1] if not build else refs[-2]
    sub = out.shape[1]

    def total(k, d, cols):
        part = keep[k, d, :sub, cols] + r0[k, d, :sub, cols].astype(jnp.float32)
        part = part + r1[k, d, :sub, cols].astype(jnp.float32)
        return part + r2[k, d, :, cols].astype(jnp.float32)

    if build:
        for d in range(depth):
            squares = total(0, d, slice(width, width + LANES))
            refs[-1][d] = lax.rsqrt(squares / features + EPS)
        scales = [refs[-1].at[d] for d in range(depth)]
    else:
        scales = [ref.at[d] for ref in refs[4:-1] for d in range(ref.shape[0])]

    for d in range(depth):
        scale = jnp.concatenate([scales[d][...]] * (step // LANES), axis=1)

        def body(j, carry, d=d, scale=scale):
            cols = pl.ds(pl.multiple_of(j * step, step), step)
            gate, up = total(0, d, cols) * scale, total(1, d, cols) * scale
            out[d, :, cols] = (jax.nn.silu(gate) * up).astype(out.dtype)
            return carry

        lax.fori_loop(0, width // step, body, 0)


def hidden_call(name, sums, scales, width, features, build):
    depth, sub = sums[0].shape[1], sums[3].shape[2]
    outs = [jax.ShapeDtypeStruct((depth, sub, width), jnp.bfloat16)]
    if build:
        outs.append(jax.ShapeDtypeStruct((depth, sub, LANES), jnp.float32))
    return pl.pallas_call(
        functools.partial(hidden_kernel, features, width, TILE, build, depth),
        in_specs=[VM] * (4 + len(scales)),
        out_specs=[VM] * len(outs),
        out_shape=outs,
        compiler_params=params(name),
        cost_estimate=pl.CostEstimate(
            flops=20 * depth * sub * width, bytes_accessed=1, transcendentals=0
        ),
        name="hidden",
    )(*sums, *scales)


def join_kernel(a, b, out):
    sub = a.shape[1]
    out[:, :sub, :] = a[...]
    out[:, sub:, :] = b[...]


def join_call(name, a, b):
    depth, sub, width = a.shape
    return pl.pallas_call(
        join_kernel,
        in_specs=[VM] * 2,
        out_specs=VM,
        out_shape=jax.ShapeDtypeStruct((depth, 2 * sub, width), a.dtype),
        compiler_params=params(name),
        cost_estimate=pl.CostEstimate(
            flops=2 * depth * sub * width, bytes_accessed=1, transcendentals=0
        ),
        name="join",
    )(a, b)


def down_kernel(first, count, deep, depths, has_acc, last, *refs):
    groups = [refs[4 * g : 4 * g + 4] for g in range(len(depths))]
    refs = refs[4 * len(depths) :]
    if has_acc:
        acc_in, refs = refs[0], refs[1:]
    dw, refs = refs[0], refs[1:]
    outs, (acc, lhs, buf, sem) = refs[:-4], refs[-4:]
    sub = groups[0][0].shape[1]
    rows = 4 * sub

    def copy(j):
        return pltpu.make_async_copy(
            dw.at[(first + j) * TILE : (first + j + 1) * TILE], buf.at[j % deep], sem.at[j % deep]
        )

    for j in range(min(deep, count)):
        copy(j).start()
    at = 0
    for pieces, depth in zip(groups, depths):
        for d in range(depth):
            for piece in pieces:
                lhs[at : at + sub, :] = piece[d]
                at += sub
    acc[...] = acc_in[...] if has_acc else jnp.zeros_like(acc)
    for j in range(count):
        copy(j).wait()
        acc[...] += jnp.dot(
            lhs[:, j * TILE : (j + 1) * TILE],
            buf[j % deep],
            preferred_element_type=jnp.float32,
        )
        if j + deep < count:
            copy(j + deep).start()
    if last:
        own, after, top, low, before = outs
        own[...] = acc[:rows]
        after[...] = acc[rows : 2 * rows]
        before[...] = acc[3 * rows :]
        top[...] = acc[2 * rows : 2 * rows + rows // 2].astype(jnp.bfloat16)
        low[...] = acc[2 * rows + rows // 2 : 3 * rows].astype(jnp.bfloat16)
    else:
        outs[0][...] = acc[...]


def down_call(name, groups, acc, dw, start, last):
    sub, width = groups[0][0].shape[1:]
    depths = [g[0].shape[0] for g in groups]
    depth, feat = sum(depths), dw.shape[1]
    rows, count = 4 * sub, width // TILE
    deep = min(count, 8)
    if last:
        whole = jax.ShapeDtypeStruct((rows, feat), jnp.float32)
        part = jax.ShapeDtypeStruct((rows // 2, feat), jnp.bfloat16)
        shapes = [whole, whole, part, part, whole]
    else:
        shapes = [jax.ShapeDtypeStruct((depth * rows, feat), jnp.float32)]
    pieces = [p for g in groups for p in g]
    return pl.pallas_call(
        functools.partial(down_kernel, start // TILE, count, deep, depths, acc is not None, last),
        in_specs=[VM] * (len(pieces) + (acc is not None)) + [HBM],
        out_specs=[VM] * len(shapes),
        out_shape=shapes,
        scratch_shapes=[
            pltpu.VMEM((depth * rows, feat), jnp.float32),
            pltpu.VMEM((depth * rows, width), jnp.bfloat16),
            pltpu.VMEM((deep, TILE, feat), jnp.bfloat16),
            pltpu.SemaphoreType.DMA((deep,)),
        ],
        compiler_params=params(name),
        cost_estimate=pl.CostEstimate(
            flops=2 * depth * rows * feat * width,
            bytes_accessed=2 * feat * width,
            transcendentals=0,
        ),
        name="down",
    )(*pieces, *([acc] if acc is not None else []), dw)


def received(kept, *arrived):
    total = kept.astype(jnp.float32)
    for a in arrived:
        total = total + a.astype(jnp.float32)
    return total.astype(jnp.bfloat16)


def fast(near_cols, n, m, patches, norm_gain, gate_weight, up_weight, down_weight):
    me = lax.axis_index("gx")
    rows, feat = patches.shape
    sub = rows // n
    features = feat * n
    ff = gate_weight.shape[1]
    others = [take(patches, d, m) for d in (1, 2, 3)]
    offs = jnp.stack([owner(me, p) for p in range(n)]).astype(jnp.int32) * sub
    gain = norm_gain.reshape(1, feat)

    def item(c, inputs, start, width, depth, scales, kind=jnp.bfloat16):
        build = c < 2
        made = up_call(
            f"up{c}", inputs, gate_weight, up_weight, start, width, (depth, rows, sub), build, kind
        )
        send, keep = made[:2]
        r0 = swap(send, 0, n)
        h = rows // 4
        r1 = swap(received(keep[:, :, h:], r0[:, :, h:]), 1, n)
        q = h // 2
        r2 = swap(received(keep[:, :, q:h], r0[:, :, q:h], r1[:, :, q:]), 2, n)
        hid = hidden_call(f"hid{c}", [keep, r0, r1, r2], scales, width, features, build)
        near = join_call(f"near{c}", hid[0], swap(hid[0], 2, n))
        far = swap(near, 1, n)
        pieces = [near, far, swap(near, 0, n), swap(far, 0, n)]
        return pieces, made[2:], hid[1:]

    p0, lhs0, scale0 = item(0, [offs, gain, patches], 0, near_cols, 1, [])
    p1, lhs1, scale1 = item(1, [offs, gain, *others], 0, near_cols, m - 1, [])
    p2, _, _ = item(
        2, [*lhs0, *lhs1], near_cols, ff - near_cols, m, [*scale0, *scale1], jnp.float32
    )
    acc = down_call("down1", [p0, p1], None, down_weight, 0, False)[0]
    own, after, top, low, before = down_call("down2", [p2], acc, down_weight, near_cols, True)
    empty = jnp.zeros_like(top)
    after = received(after, jnp.concatenate([take(top, m - 1, m), empty]))
    before = received(before, jnp.concatenate([empty, take(low, 1, m)]))
    total = own + take(after, m - 1, m).astype(jnp.float32)
    total = total + take(before, 1, m).astype(jnp.float32)
    blocks = total.reshape(n, sub, -1)
    return (
        jnp.concatenate(
            [lax.dynamic_slice_in_dim(blocks, position(me, j), 1, 0) for j in range(n)], axis=0
        )
        .reshape(rows, -1)
        .astype(jnp.bfloat16)
    )


def solution(mesh):
    n, m = mesh.shape["gx"], mesh.shape["gy"]
    placed = (P("gy", "gx"), P("gx"), P("gx", "gy"), P("gx", "gy"), P("gy", "gx"))

    def per_device(patches, norm_gain, gate_weight, up_weight, down_weight):
        rows, ff = patches.shape[0], gate_weight.shape[1]
        tiles = ff // TILE
        fits = n == 8 and m == 4 and rows % (8 * n) == 0 and ff % TILE == 0 and tiles >= 3
        if not fits:
            return generic(patches, norm_gain, gate_weight, up_weight, down_weight)
        near_cols = (tiles * 9 // 14) * TILE
        return fast(near_cols, n, m, patches, norm_gain, gate_weight, up_weight, down_weight)

    return jax.shard_map(
        per_device, mesh=mesh, in_specs=placed, out_specs=P("gy", "gx"), check_vma=False
    )
```
